32 devices in a mesh: dp: 2 (over x), ep: 4 (over z), tp: 4 (over y, core).
Axes of the slice: x: 2, y: 2, z: 4, core: 2. Of those that a mesh axis runs over, the one named last changes fastest.
Arguments:
- tokens: bfloat16 [1536, 2560], P(('dp', 'ep', 'tp')), parts along dimension 0
- expert_ids: int32 [1536, 6], P(('dp', 'ep', 'tp')), parts along dimension 0
- gate_vals: float32 [1536, 6], P(('dp', 'ep', 'tp')), parts along dimension 0
- w_gate: bfloat16 [64, 2560, 1536], P('ep', None, 'tp')
- w_up: bfloat16 [64, 2560, 1536], P('ep', None, 'tp')
- w_down: bfloat16 [64, 1536, 2560], P('ep', 'tp')
Outputs:
- output: bfloat16 [1536, 2560], P(('dp', 'ep', 'tp')), parts along dimension 0
There are 2 independent parts. The reference program is written for one: setup_inputs(seed, part) draws one part's arguments, and reference() takes and returns one part's arrays. A program takes and returns all parts, laid end to end along the dimension named above; an argument that names none is the same for every part.
All inputs are finite; a program needn't handle non-finite values.
Results may differ from the reference program's by a relative error of at most 0.0101411.
Values are sent between devices in bfloat16 or wider.
A program may use at most 1 GiB of HBM per device.

```python
import jax
import jax.numpy as jnp
from jax import lax

DMODEL = 2560
FFN = 1536
EXPERTS = 64
TOP = 6
TOK_LOC = 48
CAP_FACTOR = 2
EXPERT_RANKS = 4
TENSOR_RANKS = 4

NUM_DEV = EXPERT_RANKS * TENSOR_RANKS
CAPACITY = CAP_FACTOR * TOP * TOK_LOC // EXPERTS
HOT_ROWS = CAPACITY + 1


def routing_draw(key_route, key_hot):
    scores = jax.random.randint(key_route, (NUM_DEV, TOK_LOC, EXPERTS), 0, 65536)
    scores = scores * EXPERTS + jnp.arange(EXPERTS, dtype=jnp.int32)
    hot_ids = jax.random.randint(key_hot, (NUM_DEV, 1, 1), 0, EXPERTS)
    forced = (jnp.arange(TOK_LOC)[None, :, None] < HOT_ROWS) & (jnp.arange(EXPERTS)[None, None, :] == hot_ids)
    scores = scores + jnp.where(forced, 16777216, 0)
    chosen = lax.top_k(scores, TOP)[1]
    return chosen.reshape(NUM_DEV * TOK_LOC, TOP).astype(jnp.int32)


def setup_inputs(seed: int = 0, part: int = 0) -> dict:
    subkeys = jax.random.split(jax.random.key(seed), 8)
    key_tok = jax.random.fold_in(subkeys[0], part)
    key_route = jax.random.fold_in(subkeys[1], part)
    key_hot = jax.random.fold_in(subkeys[2], part)
    key_gate = jax.random.fold_in(subkeys[3], part)
    row_count = NUM_DEV * TOK_LOC
    tokens = jax.random.normal(key_tok, (row_count, DMODEL), jnp.float32).astype(jnp.bfloat16)
    expert_ids = routing_draw(key_route, key_hot)
    gate_vals = (0.5 + jax.random.uniform(key_gate, (row_count, TOP), jnp.float32)) * TOP ** -0.5
    w_gate = (jax.random.normal(subkeys[4], (EXPERTS, DMODEL, FFN), jnp.float32) * DMODEL ** -0.5).astype(jnp.bfloat16)
    w_up = (jax.random.normal(subkeys[5], (EXPERTS, DMODEL, FFN), jnp.float32) * DMODEL ** -0.5).astype(jnp.bfloat16)
    w_down = (jax.random.normal(subkeys[6], (EXPERTS, FFN, DMODEL), jnp.float32) * FFN ** -0.5).astype(jnp.bfloat16)
    return {"tokens": tokens, "expert_ids": expert_ids, "gate_vals": gate_vals, "w_gate": w_gate, "w_up": w_up, "w_down": w_down}


def slot_table(ids_one):
    flat_ids = ids_one.reshape(TOK_LOC * TOP)
    one_hot = (flat_ids[:, None] == jnp.arange(EXPERTS, dtype=jnp.int32)[None, :]).astype(jnp.int32)
    preceding = jnp.cumsum(one_hot, axis=0) - one_hot
    return jnp.sum(preceding * one_hot, axis=1).reshape(TOK_LOC, TOP)


def reference(tokens, expert_ids, gate_vals, w_gate, w_up, w_down):
    ids_dev = expert_ids.reshape(NUM_DEV, TOK_LOC, TOP)
    slot_ids = jax.vmap(slot_table)(ids_dev)
    kept_mask = slot_ids < CAPACITY
    dev_index = jnp.arange(NUM_DEV, dtype=jnp.int32)[:, None, None]
    tok_index = dev_index * TOK_LOC + jnp.arange(TOK_LOC, dtype=jnp.int32)[None, :, None] + jnp.zeros_like(slot_ids)
    total_slots = EXPERTS * NUM_DEV * CAPACITY
    dest_slot = jnp.where(kept_mask, (ids_dev * NUM_DEV + dev_index) * CAPACITY + slot_ids, total_slots)
    src_rows = jnp.zeros((total_slots,), jnp.int32).at[dest_slot.reshape(-1)].set(tok_index.reshape(-1), mode="drop")
    src_gate = jnp.zeros((total_slots,), jnp.float32).at[dest_slot.reshape(-1)].set(gate_vals.reshape(-1), mode="drop")

    def expert_step(acc_sum, per_expert):
        rows_idx, row_gate, wg_one, wu_one, wd_one = per_expert
        x_rows = jnp.take(tokens, rows_idx, axis=0)
        gate_pre = jnp.dot(x_rows, wg_one, preferred_element_type=jnp.float32)
        up_pre = jnp.dot(x_rows, wu_one, preferred_element_type=jnp.float32)
        hidden = (jax.nn.silu(gate_pre) * up_pre).astype(jnp.bfloat16)
        y_rows = jnp.dot(hidden, wd_one, preferred_element_type=jnp.float32).astype(jnp.bfloat16)
        acc_sum = acc_sum.at[rows_idx].add(y_rows.astype(jnp.float32) * row_gate[:, None])
        return acc_sum, None

    acc_init = jnp.zeros((NUM_DEV * TOK_LOC, DMODEL), jnp.float32)
    per_rows = src_rows.reshape(EXPERTS, NUM_DEV * CAPACITY)
    per_gate = src_gate.reshape(EXPERTS, NUM_DEV * CAPACITY)
    acc_final, _ = lax.scan(expert_step, acc_init, (per_rows, per_gate, w_gate, w_up, w_down))
    return acc_final.astype(jnp.bfloat16)
```

```python
import functools

import jax
import jax.numpy as jnp
from jax import lax
from jax.experimental import pallas as pl
from jax.experimental.pallas import tpu as pltpu
from jax.sharding import PartitionSpec as P

CAP_FACTOR = 2
ROOM = 352
ROOM_PAD = 384
COLS = 256
W_SLOTS = 5
EXT = 256
MESH = pl.DeviceIdType.MESH
BF16 = jnp.bfloat16
F32 = jnp.float32


def slot_table(ids_loc, n_exp):
    tok_loc, n_top = ids_loc.shape
    flat_ids = ids_loc.reshape(tok_loc * n_top)
    one_hot = (flat_ids[:, None] == jnp.arange(n_exp, dtype=jnp.int32)[None, :]).astype(jnp.int32)
    preceding = jnp.cumsum(one_hot, axis=0) - one_hot
    return jnp.sum(preceding * one_hot, axis=1).reshape(tok_loc, n_top)


def padded_layer(x_loc, ids_loc, gate_loc, wg_loc, wu_loc, wd_loc, expert_ranks, tensor_ranks):
    tok_loc, d_model = x_loc.shape
    n_top = ids_loc.shape[1]
    local_exp = wg_loc.shape[0]
    n_exp = local_exp * expert_ranks
    capacity = CAP_FACTOR * n_top * tok_loc // n_exp
    slot_ids = slot_table(ids_loc, n_exp)
    kept_mask = slot_ids < capacity
    flat_pos = jnp.where(kept_mask, ids_loc * capacity + slot_ids, n_exp * capacity)
    tok_index = jnp.broadcast_to(jnp.arange(tok_loc, dtype=jnp.int32)[:, None], (tok_loc, n_top))
    src_rows = jnp.zeros((n_exp * capacity,), jnp.int32).at[flat_pos.reshape(-1)].set(tok_index.reshape(-1), mode="drop")
    send_rows = jnp.take(x_loc, src_rows, axis=0).reshape(expert_ranks, local_exp, capacity, d_model)
    recv_rows = lax.all_to_all(send_rows, "ep", 0, 2, tiled=True)[0]
    copies = jnp.broadcast_to(recv_rows[None], (tensor_ranks, *recv_rows.shape))
    group_rows = lax.all_to_all(copies, "tp", 0, 2, tiled=True)[0]
    gate_pre = jnp.einsum("erd,edf->erf", group_rows, wg_loc, preferred_element_type=F32)
    up_pre = jnp.einsum("erd,edf->erf", group_rows, wu_loc, preferred_element_type=F32)
    hidden = (jax.nn.silu(gate_pre) * up_pre).astype(BF16)
    part_sums = jnp.einsum("erf,efd->erd", hidden, wd_loc, preferred_element_type=F32).astype(BF16)
    pieces = lax.all_to_all(part_sums[None], "tp", 2, 0, tiled=True)
    y_rows = jnp.sum(pieces.astype(F32), axis=0).astype(BF16)
    returned = lax.all_to_all(y_rows[None], "ep", 2, 0, tiled=True)
    y_slots = returned.reshape(n_exp * capacity, d_model)
    picked = jnp.take(y_slots, jnp.where(kept_mask, flat_pos, 0), axis=0)
    weights = jnp.where(kept_mask, gate_loc, 0.0)
    return jnp.sum(picked.astype(F32) * weights[:, :, None], axis=1).astype(BF16)


def iota(shape, dim):
    return lax.broadcasted_iota(jnp.int32, shape, dim)


def dot(a, b):
    return jnp.dot(a, b, preferred_element_type=F32)


def mask(cond):
    return jnp.where(cond, 1.0, 0.0).astype(BF16)


def layer_kernel(
    x_hbm, ids_ref, gate_ref, wg_hbm, wu_hbm, wd_hbm,
    out_ref, flag_ref,
    xall, pmat, xg, wbuf, hbuf, wdbuf, part, pack, gmat, codes, tots, flag_in,
    own, send_s, recv_s, sum_0, send_y, recv_y, ybuf, send_z, recv_z,
    sem_x, sem_w, sem_wd, sem_xr, sem_xz, sem_xy, sem_xs,
    sem_ss, sem_rs, sem_sy, sem_ry, sem_sz, sem_rz, sem_f,
):
    d_model = x_hbm.shape[1]
    tok = ids_ref.shape[0]
    n_top = ids_ref.shape[1]
    n_loc, _, f_loc = wg_hbm.shape
    n_z = xall.shape[1]
    grp = n_z * tok
    cap = CAP_FACTOR * n_top * tok // (n_loc * n_z)
    cls = n_z * cap
    crow = xg.shape[2]
    n_chunk = d_model // COLS

    dp = lax.axis_index("dp")
    z = lax.axis_index("ep")
    k = lax.axis_index("tp")
    ks = k + 1 - 2 * lax.rem(k, 2)
    ky = lax.rem(k + 2, 4)
    ksy = lax.rem(ks + 2, 4)

    def w_copy(e, half):
        slot = lax.rem(e, W_SLOTS)
        src = wg_hbm if half == 0 else wu_hbm
        dst = wbuf.at[slot, :, pl.ds(half * f_loc, f_loc)]
        return pltpu.make_async_copy(src.at[e], dst, sem_w.at[slot, half])

    def wd_copy(i):
        slot = lax.rem(i, 2)
        src = wd_hbm.at[:, :, pl.ds(pl.multiple_of(i * COLS, COLS), COLS)]
        return pltpu.make_async_copy(src, wdbuf.at[slot], sem_wd.at[slot])

    x_copy = pltpu.make_async_copy(x_hbm, xall.at[k, z, :, pl.ds(0, d_model)], sem_x)
    x_copy.start()

    @pl.loop(0, W_SLOTS)
    def _(e):
        w_copy(e, 0).start()
        w_copy(e, 1).start()

    barrier = pltpu.get_barrier_semaphore()
    for j in range(1, n_z):
        pl.semaphore_signal(barrier, inc=1, device_id={"ep": lax.rem(z + j, n_z)}, device_id_type=MESH)
    for other in (ks, ky):
        pl.semaphore_signal(barrier, inc=1, device_id={"tp": other}, device_id_type=MESH)
    pl.semaphore_signal(barrier, inc=1, device_id={"dp": 1 - dp}, device_id_type=MESH)

    lane = iota((tok, 128), 1)
    chosen = jnp.zeros((tok, 128), F32)
    gates = jnp.zeros((tok, 128), F32)
    for j in range(n_top):
        hit = ids_ref[:, j : j + 1] == lane
        chosen = jnp.where(hit, 1.0, chosen)
        gates = jnp.where(hit, gate_ref[:, j : j + 1], gates)
    before = mask(iota((tok, tok), 0) > iota((tok, tok), 1))
    slots = dot(before, chosen.astype(BF16))
    kept = jnp.logical_and(chosen > 0.5, slots < cap)
    code = jnp.where(kept, slots + (cap * z).astype(F32), -1.0)
    g1 = gates.astype(BF16).astype(F32)
    g2 = (gates - g1).astype(BF16).astype(F32)
    g3 = gates - g1 - g2
    low = lane < 64
    first = jnp.where(low, code, pltpu.roll(g1, 64, 1))
    second = jnp.where(low, g2, pltpu.roll(g3, 64, 1))
    xall[k, z, :, pl.ds(d_model, 128)] = first.astype(BF16)
    xall[k, z, :, pl.ds(d_model + 128, 128)] = second.astype(BF16)
    ybuf[...] = jnp.zeros_like(ybuf)

    x_copy.wait()
    pl.semaphore_wait(barrier, n_z + 2)

    def x_send(kk, zz, to, sem):
        blk = xall.at[kk, zz]
        return pltpu.make_async_remote_copy(
            src_ref=blk, dst_ref=blk, send_sem=sem, recv_sem=sem_xr.at[kk, zz], device_id=to, device_id_type=MESH
        )

    def x_wait(kk, zz):
        x_send(kk, zz, {"tp": ks}, sem_xs.at[0, 0]).wait_recv()

    def to_right(zz):
        return x_send(k, zz, {"ep": z + 1}, sem_xz.at[0, zz])

    def to_left(zz):
        return x_send(k, zz, {"ep": z - 1}, sem_xz.at[1, zz])

    def to_y(zz):
        return x_send(k, zz, {"tp": ky}, sem_xy.at[zz])

    def to_sib(kk, zz, row):
        return x_send(kk, zz, {"tp": ks}, sem_xs.at[row, zz])

    @pl.when(z < n_z - 1)
    def _():
        to_right(z).start()

    @pl.when(z > 0)
    def _():
        to_left(z).start()

    to_y(z).start()
    to_sib(k, z, 0).start()

    def y_arrived(zz):
        x_wait(ky, zz)
        to_sib(ky, zz, 1).start()

    for j in range(1, n_z):

        @pl.when(z - j >= 0)
        def _():
            x_wait(k, z - j)

            @pl.when(z < n_z - 1)
            def _():
                to_right(z - j).start()

            to_y(z - j).start()
            to_sib(k, z - j, 0).start()

        @pl.when(z + j < n_z)
        def _():
            x_wait(k, z + j)

            @pl.when(z > 0)
            def _():
                to_left(z + j).start()

            to_y(z + j).start()
            to_sib(k, z + j, 0).start()

        if j == 1:
            y_arrived(z)
        else:

            @pl.when(z - j + 1 >= 0)
            def _():
                y_arrived(z - j + 1)

            @pl.when(z + j - 1 < n_z)
            def _():
                y_arrived(z + j - 1)

    def gather(kk):
        ext = xall[kk, :, :, pl.ds(d_model, 128)].reshape(grp, 128)
        pick_e = mask(iota((n_loc, 128), 1) == iota((n_loc, 128), 0) + z * n_loc)
        code_t = lax.dot_general(pick_e, ext, (((1,), (1,)), ((), ())), preferred_element_type=F32)
        row = iota((n_loc, crow, grp), 1).astype(F32)
        pmat[...] = jnp.where(code_t[:, None, :] == row, 1.0, 0.0).astype(BF16).reshape(n_loc * crow, grp)

        @pl.loop(0, d_model // 512)
        def _(n):
            at = pl.ds(pl.multiple_of(n * 512, 512), 512)
            got = dot(pmat[...], xall[kk, :, :, at].reshape(grp, 512))
            xg[:, kk, :, at] = got.astype(BF16).reshape(n_loc, crow, 512)

        kept_t = mask(code_t >= 0.0)
        lane_m = iota((grp, 128), 1)
        from_z = iota((grp, 128), 0) // tok
        lane_z = lane_m // cap
        valid = lane_m < cls
        count = dot(kept_t, mask(jnp.logical_and(lane_z == from_z, valid)))
        prior_z = dot(kept_t, mask(jnp.logical_and(from_z < lane_z, valid)))
        total = dot(kept_t, jnp.ones((grp, 128), BF16))
        below = mask(iota((n_loc, n_loc), 0) > iota((n_loc, n_loc), 1))
        base = dot(below, total.astype(BF16)) + prior_z
        m_lane = iota((n_loc, 128), 1)
        slot = (m_lane - cap * (m_lane // cap)).astype(F32)
        pos = jnp.where(jnp.logical_and(slot < count, m_lane < cls), base + slot, -1.0)
        high = jnp.floor(pos * (1.0 / 32.0))
        lowp = pos - 32.0 * high
        width = n_loc * crow
        lane_w = iota((128, width), 1)
        spread = mask(lane_w - crow * (lane_w // crow) == iota((128, width), 0))
        wide = 32.0 * dot(high.astype(BF16), spread) + dot(lowp.astype(BF16), spread)
        here = iota((n_loc, width), 1) // crow == iota((n_loc, width), 0)
        pos_row = jnp.sum(jnp.where(here, wide, 0.0), axis=0, keepdims=True)
        pack[kk] = jnp.where(pos_row == iota((ROOM, width), 0).astype(F32), 1.0, 0.0).astype(BF16)

        kept_n = mask(jnp.logical_and(ext.astype(F32) >= 0.0, iota((grp, 128), 1) < 64))
        per_e = dot(jnp.ones((8, grp), BF16), kept_n)
        same = mask(iota((128, 128), 0) // n_loc == iota((128, 128), 1) // n_loc)
        return dot(per_e.astype(BF16), same)

    tot = gather(k)
    for zz in range(n_z):
        x_wait(ks, zz)
    tot = jnp.maximum(tot, gather(ks))

    @pl.when(z == 0)
    def _():
        y_arrived(n_z - 1)

    @pl.when(z == n_z - 1)
    def _():
        y_arrived(0)

    tot = jnp.maximum(tot, gather(ky))
    for zz in range(n_z):
        x_wait(ksy, zz)
    tots[...] = jnp.maximum(tot, gather(ksy))
    f_copy = pltpu.make_async_remote_copy(
        src_ref=tots, dst_ref=flag_in, send_sem=sem_f.at[0], recv_sem=sem_f.at[1],
        device_id={"dp": 1 - dp}, device_id_type=MESH,
    )

    wd_copy(0).start()
    wd_copy(1).start()

    pick_n = mask(iota((128, 128), 0) == iota((128, 128), 1) + z * n_loc)
    pick_h = mask(iota((128, 128), 0) == iota((128, 128), 1) + z * n_loc + 64)
    in_e = iota((tok, 128), 1) < n_loc
    kept_all = []
    for zz in range(n_z):
        code_n = dot(xall[k, zz, :, pl.ds(d_model, 128)], pick_n)
        kept_all.append(jnp.logical_and(code_n >= 0.0, in_e))
        codes[zz] = code_n - float(cap * zz)
    counts = [dot(jnp.ones((tok, tok), BF16), mask(kz)) for kz in kept_all]
    all_cnt = counts[0]
    for c in counts[1:]:
        all_cnt = all_cnt + c
    base_e = dot(all_cnt.astype(BF16), mask(iota((128, 128), 0) < iota((128, 128), 1)))
    prior = jnp.zeros((tok, 128), F32)
    p_lane = iota((tok, ROOM_PAD), 1).astype(F32)
    for zz in range(n_z):
        pos = jnp.where(kept_all[zz], base_e + prior + codes[zz], -1.0)
        prior = prior + counts[zz]
        e0 = xall[k, zz, :, pl.ds(d_model, 128)]
        e1 = xall[k, zz, :, pl.ds(d_model + 128, 128)]
        terms = (dot(e0, pick_h), dot(e1, pick_n), dot(e1, pick_h))
        acc = [jnp.zeros((tok, ROOM_PAD), F32) for _ in terms]
        for e in range(n_loc):
            hit = pos[:, e : e + 1] == p_lane
            acc = [jnp.where(hit, t[:, e : e + 1], a) for t, a in zip(terms, acc)]
        for i, a in enumerate(acc):
            gmat[zz, i] = a.astype(BF16)

    f_copy.start()

    @pl.loop(0, n_loc)
    def _(e):
        w_copy(e, 0).wait()
        w_copy(e, 1).wait()
        both = dot(xg[e].reshape(4 * crow, d_model), wbuf[lax.rem(e, W_SLOTS)])
        a, b = both[:, :f_loc], both[:, f_loc:]
        hbuf[e] = (a / (1.0 + jnp.exp(-a)) * b).astype(BF16)

        @pl.when(e + W_SLOTS < n_loc)
        def _():
            w_copy(e + W_SLOTS, 0).start()
            w_copy(e + W_SLOTS, 1).start()

    def s_copy(i):
        return pltpu.make_async_remote_copy(
            src_ref=send_s.at[lax.rem(i, 2)], dst_ref=recv_s.at[i], send_sem=sem_ss.at[lax.rem(i, 2)],
            recv_sem=sem_rs.at[i], device_id={"tp": ks}, device_id_type=MESH,
        )

    def y_copy(i):
        return pltpu.make_async_remote_copy(
            src_ref=send_y.at[lax.rem(i, 2)], dst_ref=recv_y.at[i], send_sem=sem_sy.at[lax.rem(i, 2)],
            recv_sem=sem_ry.at[i], device_id={"tp": ky}, device_id_type=MESH,
        )

    def z_copy(i, j):
        to = lax.rem(z + j, n_z)
        return pltpu.make_async_remote_copy(
            src_ref=send_z.at[lax.rem(i, 2), to], dst_ref=recv_z.at[i, j - 1], send_sem=sem_sz.at[lax.rem(i, 2), j - 1],
            recv_sem=sem_rz.at[i, j - 1], device_id={"ep": to}, device_id_type=MESH,
        )

    def down(i):
        par = lax.rem(i, 2)
        wd_copy(i).wait()

        @pl.loop(0, n_loc)
        def _(e):
            got = dot(hbuf[e], wdbuf[par, e])
            part[:, e] = got.astype(BF16).reshape(4, crow, COLS)

        @pl.when(i + 2 < n_chunk)
        def _():
            wd_copy(i + 2).start()

        @pl.when(i >= 2)
        def _():
            s_copy(i - 2).wait_send()

        def packed(kk):
            return dot(pack[kk], part[kk].reshape(n_loc * crow, COLS)).astype(BF16)

        send_s[par, 0] = packed(ks)
        send_s[par, 1] = packed(ksy)
        s_copy(i).start()
        own[par, 0] = packed(k)
        own[par, 1] = packed(ky)

    def across_y(i):
        par = lax.rem(i, 2)
        s_copy(i).wait_recv()

        @pl.when(i >= 2)
        def _():
            y_copy(i - 2).wait_send()

        send_y[par] = (own[par, 1].astype(F32) + recv_s[i, 1].astype(F32)).astype(BF16)
        y_copy(i).start()
        sum_0[par] = own[par, 0].astype(F32) + recv_s[i, 0].astype(F32)

    def across_z(i):
        par = lax.rem(i, 2)
        y_copy(i).wait_recv()
        ybuf[pl.ds(0, ROOM), :] = (sum_0[par] + recv_y[i].astype(F32)).astype(BF16)

        @pl.when(i >= 2)
        def _():
            for j in range(1, n_z):
                z_copy(i - 2, j).wait_send()

        got = dot(gmat[...].reshape(n_z * 3 * tok, ROOM_PAD), ybuf[...]).reshape(n_z, 3, tok, COLS)
        send_z[par] = (got[:, 2] + got[:, 1]) + got[:, 0]
        for j in range(1, n_z):
            z_copy(i, j).start()

    def finish(i):
        for j in range(1, n_z):
            z_copy(i, j).wait_recv()
        out = send_z[lax.rem(i, 2), z]
        for j in range(1, n_z):
            out = out + recv_z[i, j - 1]
        out_ref[:, pl.ds(pl.multiple_of(i * COLS, COLS), COLS)] = out.astype(BF16)

    @pl.loop(0, n_chunk + 3)
    def _(it):
        @pl.when(it < n_chunk)
        def _():
            down(it)

        @pl.when(jnp.logical_and(it >= 1, it < n_chunk + 1))
        def _():
            across_y(it - 1)

        @pl.when(jnp.logical_and(it >= 2, it < n_chunk + 2))
        def _():
            across_z(it - 2)

        @pl.when(it >= 3)
        def _():
            finish(it - 3)

    f_copy.wait()
    flag_ref[...] = jnp.maximum(tots[...], flag_in[...])
    for i in (n_chunk - 2, n_chunk - 1):
        s_copy(i).wait_send()
        y_copy(i).wait_send()
        for j in range(1, n_z):
            z_copy(i, j).wait_send()

    @pl.loop(0, n_z)
    def _(zz):
        @pl.when(jnp.logical_and(z < n_z - 1, zz <= z))
        def _():
            to_right(zz).wait_send()

        @pl.when(jnp.logical_and(z > 0, zz >= z))
        def _():
            to_left(zz).wait_send()

        to_y(zz).wait_send()
        to_sib(k, zz, 0).wait_send()
        to_sib(ky, zz, 1).wait_send()


def packed_layer(n_z, x_loc, ids_loc, gate_loc, wg_loc, wu_loc, wd_loc):
    tok, d_model = x_loc.shape
    n_loc, _, f_loc = wg_loc.shape
    n_top = ids_loc.shape[1]
    cap = CAP_FACTOR * n_top * tok // (n_loc * n_z)
    crow = -(-n_z * cap // 16) * 16
    n_chunk = d_model // COLS
    wide = d_model + EXT
    dma = pltpu.SemaphoreType.DMA
    return pl.pallas_call(
        layer_kernel,
        out_shape=(jax.ShapeDtypeStruct((tok, d_model), BF16), jax.ShapeDtypeStruct((8, 128), F32)),
        in_specs=[
            pl.BlockSpec(memory_space=pl.ANY),
            pl.BlockSpec(memory_space=pltpu.VMEM),
            pl.BlockSpec(memory_space=pltpu.VMEM),
            pl.BlockSpec(memory_space=pl.ANY),
            pl.BlockSpec(memory_space=pl.ANY),
            pl.BlockSpec(memory_space=pl.ANY),
        ],
        out_specs=(pl.BlockSpec(memory_space=pltpu.VMEM), pl.BlockSpec(memory_space=pltpu.VMEM)),
        scratch_shapes=[
            pltpu.VMEM((4, n_z, tok, wide), BF16),
            pltpu.VMEM((n_loc * crow, n_z * tok), BF16),
            pltpu.VMEM((n_loc, 4, crow, d_model), BF16),
            pltpu.VMEM((W_SLOTS, d_model, 2 * f_loc), BF16),
            pltpu.VMEM((n_loc, 4 * crow, f_loc), BF16),
            pltpu.VMEM((2, n_loc, f_loc, COLS), BF16),
            pltpu.VMEM((4, n_loc, crow, COLS), BF16),
            pltpu.VMEM((4, ROOM, n_loc * crow), BF16),
            pltpu.VMEM((n_z, 3, tok, ROOM_PAD), BF16),
            pltpu.VMEM((n_z, tok, 128), F32),
            pltpu.VMEM((8, 128), F32),
            pltpu.VMEM((8, 128), F32),
            pltpu.VMEM((2, 2, ROOM, COLS), BF16),
            pltpu.VMEM((2, 2, ROOM, COLS), BF16),
            pltpu.VMEM((n_chunk, 2, ROOM, COLS), BF16),
            pltpu.VMEM((2, ROOM, COLS), F32),
            pltpu.VMEM((2, ROOM, COLS), BF16),
            pltpu.VMEM((n_chunk, ROOM, COLS), BF16),
            pltpu.VMEM((ROOM_PAD, COLS), BF16),
            pltpu.VMEM((2, n_z, tok, COLS), F32),
            pltpu.VMEM((n_chunk, n_z - 1, tok, COLS), F32),
            dma,
            dma((W_SLOTS, 2)),
            dma((2,)),
            dma((4, n_z)),
            dma((2, n_z)),
            dma((n_z,)),
            dma((2, n_z)),
            dma((2,)),
            dma((n_chunk,)),
            dma((2,)),
            dma((n_chunk,)),
            dma((2, n_z - 1)),
            dma((n_chunk, n_z - 1)),
            dma((2,)),
        ],
        compiler_params=pltpu.CompilerParams(collective_id=0, has_side_effects=True, vmem_limit_bytes=67043328),
        name="moe_layer",
    )(x_loc, ids_loc, gate_loc, wg_loc, wu_loc, wd_loc)


def solution(mesh):
    expert_ranks, tensor_ranks = mesh.shape["ep"], mesh.shape["tp"]
    row_spec = P(("dp", "ep", "tp"), None)

    def local_layer(*args):
        out, totals = packed_layer(expert_ranks, *args)
        fits = jnp.max(totals) <= ROOM
        return lax.cond(
            fits,
            lambda out, *args: out,
            lambda out, *args: padded_layer(*args, expert_ranks, tensor_ranks),
            out,
            *args,
        )

    return jax.shard_map(local_layer, mesh=mesh, in_specs=(row_spec, row_spec, row_spec, P("ep", None, "tp"), P("ep", None, "tp"), P("ep", "tp", None)), out_specs=row_spec, check_vma=False)
```
